768 devices in a mesh: face: 12 (over z), tile: 64 (over x, y, core).
Axes of the slice: x: 4, y: 8, z: 12, core: 2. Of those that a mesh axis runs over, the one named last changes fastest.
Arguments:
- tracers: float32 [48, 256, 16, 1280], P('face', 'tile'), may hold values from -6 to 6
- basis_weights: float32 [2, 48, 256, 16, 16], P(None, 'face', 'tile'), may hold values from -1 to 1
- up_owner: int32 [2, 48, 256], P(None, 'face', 'tile'), may hold values from 0 to 4, as said below
- up_slot: int32 [2, 48, 256], P(None, 'face', 'tile'), may hold values from 0 to 15, as said below
- send_list: int32 [2, 48, 256], replicated, may hold values from 0 to 15, as said below
Outputs:
- transported: float32 [48, 256, 16, 1280], P('face', 'tile')
The draws below stay inside these ranges and needn't reach their ends.
Inputs may be any that keep to these rules, and one draw needn't show every extreme that they name: `up_owner`: 0: the upstream element is on the same device; 1 and 2: on the device before or after along face, cyclically; 3 and 4: before or after along tile. On one device in one step, each position of each neighbour's list toward it is named by at most one target element, and a device names positions 0 to k - 1 of a list, k between 1 and 4, with 4 reached in every draw. `up_slot`: below 4 where up_owner is not 0. `send_list`: entry [s, 4 f + j, 4 t + c] is the c-th local element that device (f, t) lists in step s for direction j (j = 0: toward face + 1, 1: toward face - 1, 2: toward tile + 1, 3: toward tile - 1); the entries of one list are distinct.
All inputs are finite; a program needn't handle non-finite values.
Results may differ from the reference program's by a relative error of at most 0.0001.
Values sent between devices are 32-bit elements; how exact they have to be, the bound alone decides.
No kernel may reach another device: no remote copies, remote signals or barrier semaphores. Data moves between devices by JAX's collectives and lax.ppermute only.
A program may use at most 64 MiB of HBM per device.

```python
import jax
import jax.numpy as jnp
from jax import lax

TRACERS = 10
LEVELS = 128
NODES = 16
EDGE = 4
STEPS = 2
CAP = 4
NEX = 48
NEY = 256
N_FACE = 12
N_TILE = 64


def lagrange_rows(points):
    gll_nodes = [-1.0, -0.4472135955, 0.4472135955, 1.0]
    columns = []
    for first in range(4):
        term = jnp.ones_like(points)
        for other in range(4):
            if other != first:
                term = term * (points - gll_nodes[other]) / (gll_nodes[first] - gll_nodes[other])
        columns.append(term)
    return jnp.stack(columns, axis=-1)


def draw_basis_weights(key, part):
    key_x, key_y = jax.random.split(jax.random.fold_in(key, 11))
    shape = (STEPS, NEX, NEY, 16)
    points_x = jax.random.uniform(key_x, shape, jnp.float32, -1.0, 1.0)
    points_y = jax.random.uniform(key_y, shape, jnp.float32, -1.0, 1.0)
    basis_x = lagrange_rows(points_x)
    basis_y = lagrange_rows(points_y)
    product = basis_x[..., :, None] * basis_y[..., None, :]
    return product.reshape(STEPS, NEX, NEY, 16, 16).astype(jnp.float32)


def draw_routes(key):
    base = jax.random.fold_in(key, 7)
    key_count, key_order, key_own = jax.random.split(base, 3)
    elem_count = EDGE * EDGE
    counts = jax.random.randint(key_count, (STEPS, N_FACE, N_TILE, 4), 1, CAP + 1).astype(jnp.int32)
    counts = counts.at[:, 0, 0, 0].set(CAP)
    counts = counts.at[:, 0, 1, 0].set(max(CAP - 1, 1))
    scores = jax.random.randint(key_order, (STEPS, N_FACE, N_TILE, elem_count), 0, 1 << 20) * elem_count
    scores = scores + jnp.arange(elem_count, dtype=jnp.int32)
    order = jnp.argsort(scores, axis=-1)
    ranks = jnp.argsort(order, axis=-1).astype(jnp.int32)
    ends = jnp.cumsum(counts, axis=-1).astype(jnp.int32)
    starts = ends - counts
    passed = jnp.sum((ranks[..., None] >= ends[..., None, :]).astype(jnp.int32), axis=-1)
    remote = ranks < ends[..., 3:4]
    owners = jnp.where(remote, passed + 1, 0).astype(jnp.int32)
    start_of = jnp.take_along_axis(starts, jnp.minimum(passed, 3), axis=-1)
    own_slot = jax.random.randint(key_own, (STEPS, N_FACE, N_TILE, elem_count), 0, elem_count)
    own_slot = jnp.where(ranks == ends[..., 3:4], elem_count - 1, own_slot)
    slots = jnp.where(remote, ranks - start_of, own_slot).astype(jnp.int32)

    def layout(values):
        values = values.reshape(STEPS, N_FACE, N_TILE, EDGE, EDGE).transpose(0, 1, 3, 2, 4)
        return values.reshape(STEPS, NEX, NEY)
    return (layout(owners), layout(slots))


def draw_up_owner(key, part):
    return draw_routes(key)[0]


def draw_up_slot(key, part):
    return draw_routes(key)[1]


def draw_send_list(key, part):
    elem_count = EDGE * EDGE
    scores = jax.random.randint(jax.random.fold_in(key, 3), (STEPS, N_FACE, 4, N_TILE, elem_count), 0, 1 << 20)
    scores = scores * elem_count + jnp.arange(elem_count, dtype=jnp.int32)
    order = jnp.argsort(scores, axis=-1)[..., :CAP].astype(jnp.int32)
    return order.reshape(STEPS, 4 * N_FACE, N_TILE * CAP)


def block_levels(rng, dims, cuts, least, top_value):
    level, own = 1.0, jax.random.fold_in(rng, 6)
    for position, shards_of in cuts:
        heights = jnp.exp(jax.random.uniform(jax.random.fold_in(own, position), (shards_of,), jnp.float32, least / len(cuts), top_value / len(cuts)))
        level = level * jnp.repeat(heights, dims[position] // shards_of).reshape([-1 if axis == position else 1 for axis in range(len(dims))])
    return level


def scatter_about(rng, shape, spread, bound, cuts=(), kind=jnp.bfloat16):
    loudness = block_levels(rng, shape, cuts, -0.22, 0.18) if cuts else 1.0
    drawn = jax.random.normal(rng, shape, jnp.float32) * spread * loudness
    return jnp.minimum(jnp.maximum(drawn, -bound), bound).astype(kind)


def setup_inputs(seed: int = 0) -> dict:
    arg_keys = jax.random.split(jax.random.key(seed), 6)
    return {
        "tracers": scatter_about(arg_keys[0], (NEX, NEY, NODES, TRACERS * LEVELS), 1.0, 6.0, ((0, 12), (1, 64)), jnp.float32),
        "basis_weights": draw_basis_weights(jax.random.fold_in(arg_keys[5], 71), 0),
        "up_owner": draw_up_owner(jax.random.fold_in(arg_keys[5], 71), 0),
        "up_slot": draw_up_slot(jax.random.fold_in(arg_keys[5], 71), 0),
        "send_list": draw_send_list(jax.random.fold_in(arg_keys[5], 71), 0),
    }


def average_edges(interpolated):
    elem_rows = interpolated.shape[0]
    elem_cols = interpolated.shape[1]
    columns = interpolated.shape[3]
    node_grid = interpolated.reshape(elem_rows, elem_cols, 4, 4, columns).transpose(0, 2, 1, 3, 4)
    node_grid = node_grid.reshape(4 * elem_rows, 4 * elem_cols, columns)
    row_pos = jnp.arange(4 * elem_rows, dtype=jnp.int32) % 4
    at_first = (row_pos == 0)[:, None, None]
    at_last = (row_pos == 3)[:, None, None]
    row_pass = jnp.where(at_first, 0.5 * (node_grid + jnp.roll(node_grid, 1, 0)),
                         jnp.where(at_last, 0.5 * (node_grid + jnp.roll(node_grid, -1, 0)), node_grid))
    col_pos = jnp.arange(4 * elem_cols, dtype=jnp.int32) % 4
    col_first = (col_pos == 0)[None, :, None]
    col_last = (col_pos == 3)[None, :, None]
    col_pass = jnp.where(col_first, 0.5 * (row_pass + jnp.roll(row_pass, 1, 1)),
                         jnp.where(col_last, 0.5 * (row_pass + jnp.roll(row_pass, -1, 1)), row_pass))
    col_pass = col_pass.reshape(elem_rows, 4, elem_cols, 4, columns).transpose(0, 2, 1, 3, 4)
    return col_pass.reshape(elem_rows, elem_cols, 16, columns)


def reference(tracers, basis_weights, up_owner, up_slot, send_list):
    device_face = (jnp.arange(NEX, dtype=jnp.int32) // EDGE)[:, None]
    device_tile = (jnp.arange(NEY, dtype=jnp.int32) // EDGE)[None, :]
    tracer_field = tracers
    for sweep_index in range(STEPS):
        owners = up_owner[sweep_index]
        slot_index = up_slot[sweep_index]
        owner_face = jnp.where(owners == 1, (device_face - 1) % N_FACE,
                               jnp.where(owners == 2, (device_face + 1) % N_FACE, device_face))
        owner_tile = jnp.where(owners == 3, (device_tile - 1) % N_TILE,
                               jnp.where(owners == 4, (device_tile + 1) % N_TILE, device_tile))
        owner_face = owner_face.astype(jnp.int32)
        owner_tile = owner_tile.astype(jnp.int32)
        listed = send_list[sweep_index][owner_face * 4 + jnp.maximum(owners - 1, 0),
                                        owner_tile * CAP + jnp.minimum(slot_index, CAP - 1)]
        local_elem = jnp.where(owners == 0, slot_index, listed).astype(jnp.int32)
        source = tracer_field[owner_face * EDGE + local_elem // EDGE, owner_tile * EDGE + local_elem % EDGE]
        interpolated = jnp.einsum("xyij,xyjc->xyic", basis_weights[sweep_index], source,
                                  precision=lax.Precision.HIGHEST)
        interpolated = jnp.clip(interpolated, jnp.min(source, axis=2, keepdims=True),
                                jnp.max(source, axis=2, keepdims=True))
        tracer_field = average_edges(interpolated)
    return tracer_field
```

```python
import functools

import jax
import jax.numpy as jnp
from jax import lax
from jax.experimental import pallas as pl
from jax.experimental.pallas import tpu as pltpu
from jax.sharding import PartitionSpec as P

F32 = jnp.float32
BF16 = jnp.bfloat16
VMEM = pl.BlockSpec(memory_space=pltpu.VMEM)
SMEM = pl.BlockSpec(memory_space=pltpu.SMEM)
HBM = pl.BlockSpec(memory_space=pltpu.HBM)
ELEMS = 16
NODES = 16
CAP = 4


def cost(cycles_bytes):
    return pl.CostEstimate(flops=0, transcendentals=0, bytes_accessed=cycles_bytes)


def grant(mib):
    return pltpu.CompilerParams(vmem_limit_bytes=mib << 20)


def list_copy(step, lists, table, sem):
    rows, cols = table.shape
    row = lax.axis_index("face") * 4
    col = lax.axis_index("tile") * CAP
    row0, col0 = lax.div(row, rows) * rows, lax.div(col, cols) * cols
    copy = pltpu.make_async_copy(
        lists.at[step, pl.ds(pl.multiple_of(row0, rows), rows), pl.ds(pl.multiple_of(col0, cols), cols)],
        table,
        sem,
    )
    return copy, row - row0, col - col0


def directions():
    return odd("face"), 1 - odd("face"), 2 + odd("tile"), 3 - odd("tile")


def first_gather(lists, field, *rest):
    sends, (table, list_sem, sems) = rest[:4], rest[4:]
    copy, row, col = list_copy(0, lists, table, list_sem)
    copy.start()
    copy.wait()
    copies = []
    for k, j in enumerate(directions()):
        for c in range(CAP):
            copies.append(
                pltpu.make_async_copy(
                    field.at[table[row + j, col + c]], sends[k].at[c], sems.at[k * CAP + c]
                )
            )
            copies[-1].start()
    for copy in copies:
        copy.wait()


def spread_weights(weights, high, low):
    lane = lax.broadcasted_iota(jnp.int32, (16, 256), 1)
    row = lax.broadcasted_iota(jnp.int32, (16, 256), 0)
    spread = jnp.where(lane % 16 == row, 1.0, 0.0).astype(BF16)
    out_row = lax.broadcasted_iota(jnp.int32, (256, 256), 0)
    out_col = lax.broadcasted_iota(jnp.int32, (256, 256), 1)
    own = out_row // 16 == out_col // 16
    for step in range(weights.shape[0]):
        w = weights[step]
        w_high = w.astype(BF16)
        w_low = (w - w_high.astype(F32)).astype(BF16)
        for part, out in ((w_high, high), (w_low, low)):
            wide = jnp.dot(part, spread, preferred_element_type=F32)
            out[step] = jnp.where(own, wide, 0.0).astype(BF16)


def sublane(shape=(8, 1)):
    return lax.broadcasted_iota(jnp.int32, shape, 0)


def roll(x, by):
    return x if by % 8 == 0 else pltpu.roll(x, by % 8, 0)


def move(step, owner, slot, field, face_first, face_second, tile_first, tile_second, high, low,
         moved, row_first, row_second, source, split_high, split_low):
    owners = (2 - odd("face"), 1 + odd("face"), 4 - odd("tile"), 3 + odd("tile"))
    for e in range(ELEMS):
        o = owner[step, e // 4, e % 4]
        p = slot[step, e // 4, e % 4]
        c = jnp.minimum(p, CAP - 1)
        block = field[p]
        for code, arrived in zip(owners, (face_first, face_second, tile_first, tile_second)):
            block = jnp.where(o == code, arrived[c], block)
        source[e] = block
        part = block.astype(BF16)
        split_high[pl.ds(e * 16, 16), :] = part
        split_low[pl.ds(e * 16, 16), :] = (block - part.astype(F32)).astype(BF16)
    wide = 256
    for n in range(0, field.shape[2], wide):
        cols = pl.ds(n, wide)
        s_high, s_low = split_high[:, cols], split_low[:, cols]
        w_high, w_low = high[step], low[step]
        total = jnp.dot(w_high, s_high, preferred_element_type=F32)
        total += jnp.dot(w_high, s_low, preferred_element_type=F32)
        total += jnp.dot(w_low, s_high, preferred_element_type=F32)
        for e in range(ELEMS):
            src = source[e, :, cols]
            least = jnp.min(src, axis=0, keepdims=True)
            most = jnp.max(src, axis=0, keepdims=True)
            moved[e, :, cols] = jnp.clip(total[e * 16 : e * 16 + 16], least, most)
    sub = sublane()
    packed = []
    for x, tile in ((0, 0), (3, 1)):
        rows = []
        for pair in range(2):
            even = moved[4 * x + 2 * pair, 8 * tile : 8 * tile + 8, :]
            after = moved[4 * x + 2 * pair + 1, 8 * tile : 8 * tile + 8, :]
            if tile == 0:
                rows.append(jnp.where(sub < 4, even, roll(after, 4)))
            else:
                rows.append(jnp.where(sub < 4, roll(even, 4), after))
        left, right = rows
        inner = []
        for t in rows:
            t2 = jnp.where(sub == 3, 0.5 * (t + roll(t, 7)), t)
            inner.append(jnp.where(sub == 4, 0.5 * (t + roll(t, 1)), t2))
        inner[0] = jnp.where(sub == 7, 0.5 * (left + roll(right, 7)), inner[0])
        inner[1] = jnp.where(sub == 0, 0.5 * (right + roll(left, 1)), inner[1])
        packed.append(inner)
    flip = odd("face") == 1
    for k in range(2):
        rows = slice(8 * k, 8 * k + 8)
        top, bottom = packed[0][k], packed[1][k]
        row_first[rows, :] = jnp.where(flip, top, bottom)
        row_second[rows, :] = jnp.where(flip, bottom, top)


def average_inside(moved, inside, left, right, draft):
    sub = sublane()
    first, last = sub % 4 == 0, sub % 4 == 3
    for e in range(ELEMS):
        y = e % 4
        for k in range(2):
            rows = slice(8 * k, 8 * k + 8)
            m = moved[e, rows, :]
            c = m
            if y < 3:
                c = jnp.where(last, 0.5 * (m + roll(moved[e + 1, rows, :], 3)), c)
            if y > 0:
                c = jnp.where(first, 0.5 * (m + roll(moved[e - 1, rows, :], 5)), c)
            draft[e, rows, :] = c
    for e in range(ELEMS):
        x = e // 4
        t0, t1 = draft[e, 0:8, :], draft[e, 8:16, :]
        if x > 0:
            t0 = jnp.where(sub < 4, 0.5 * (t0 + roll(draft[e - 4, 8:16, :], 4)), t0)
        if x < 3:
            t1 = jnp.where(sub >= 4, 0.5 * (t1 + roll(draft[e + 4, 0:8, :], 4)), t1)
        inside[e, 0:8, :] = t0
        inside[e, 8:16, :] = t1
    for out, y, at in ((left, 0, 0), (right, 3, 3)):
        for pair in range(2):
            packed = None
            for place in range(4):
                e = 4 * (2 * pair + place // 2) + y
                k = place % 2
                t = roll(inside[e, 8 * k : 8 * k + 8, :], place - at)
                packed = t if packed is None else jnp.where(sub % 4 == place, t, packed)
            out[8 * pair : 8 * pair + 8, :] = packed


def finish_columns(left, right, face_first, face_second, column_first, column_second):
    sub = sublane()
    flip = odd("face") == 1
    lo, hi = slice(0, 8), slice(8, 16)
    a0, a1, b0, b1 = (
        jnp.where(flip == from_first, face_first[rows, :], face_second[rows, :])
        for from_first in (True, False)
        for rows in (lo, hi)
    )
    l0 = jnp.where(sub == 0, 0.5 * (left[lo, :] + a0), left[lo, :])
    l1 = jnp.where(sub == 7, 0.5 * (left[hi, :] + roll(b0, 7)), left[hi, :])
    r0 = jnp.where(sub == 0, 0.5 * (right[lo, :] + roll(a1, 1)), right[lo, :])
    r1 = jnp.where(sub == 7, 0.5 * (right[hi, :] + b1), right[hi, :])
    flip = odd("tile") == 1
    for rows, l, r in ((lo, l0, r0), (hi, l1, r1)):
        column_first[rows, :] = jnp.where(flip, l, r)
        column_second[rows, :] = jnp.where(flip, r, l)


def finish_rows(inside, face_first, face_second, out):
    sub = sublane()
    flip = odd("face") == 1
    out[4:12] = inside[4:12]
    for y in range(4):
        first = face_first[8 * (y // 2) : 8 * (y // 2) + 8, :]
        second = face_second[8 * (y // 2) : 8 * (y // 2) + 8, :]
        a, b = jnp.where(flip, first, second), jnp.where(flip, second, first)
        t = inside[y, 0:8, :]
        out[y, 0:8, :] = jnp.where(sub < 4, 0.5 * (t + roll(a, 4 * (y % 2))), t)
        out[y, 8:16, :] = inside[y, 8:16, :]
        out[12 + y, 0:8, :] = inside[12 + y, 0:8, :]
        t = inside[12 + y, 8:16, :]
        out[12 + y, 8:16, :] = jnp.where(sub >= 4, 0.5 * (t + roll(b, 4 - 4 * (y % 2))), t)


def fix_edges(inside, tile_first, tile_second, out):
    sub = sublane()
    first, last = sub % 4 == 0, sub % 4 == 3
    flip = odd("tile") == 1
    for x in range(4):
        one = tile_first[8 * (x // 2) : 8 * (x // 2) + 8, :]
        two = tile_second[8 * (x // 2) : 8 * (x // 2) + 8, :]
        before, after = jnp.where(flip, one, two), jnp.where(flip, two, one)
        out[4 * x + 1 : 4 * x + 3] = inside[4 * x + 1 : 4 * x + 3]
        for k in range(2):
            place = 2 * (x % 2) + k
            rows = slice(8 * k, 8 * k + 8)
            t = inside[4 * x, rows, :]
            out[4 * x, rows, :] = jnp.where(first, 0.5 * (t + roll(before, -place)), t)
            t = inside[4 * x + 3, rows, :]
            out[4 * x + 3, rows, :] = jnp.where(last, 0.5 * (t + roll(after, 3 - place)), t)


def finish_field(step, lists, inside, tile_first, tile_second, field, *rest):
    sends, (table, list_sem) = rest[:4], rest[4:]
    copy, row, col = list_copy(step + 1, lists, table, list_sem)
    copy.start()
    fix_edges(inside, tile_first, tile_second, field)
    copy.wait()
    for k, j in enumerate(directions()):
        for c in range(CAP):
            sends[k][c] = field[table[row + j, col + c]]


def finish_last(inside, tile_first, tile_second, field):
    fix_edges(inside, tile_first, tile_second, field)


def swap(axis, offset, x):
    count = lax.axis_size(axis)
    pairs = []
    for i in range(offset, count + offset, 2):
        pairs += [(i % count, (i + 1) % count), ((i + 1) % count, i % count)]
    return lax.ppermute(x, axis, sorted(pairs))


def swaps(axis, first, second):
    return swap(axis, 0, first), swap(axis, 1, second)


def odd(axis):
    return lax.rem(lax.axis_index(axis), 2)


def local(tracers, basis_weights, up_owner, up_slot, send_list):
    columns = tracers.shape[3]
    steps = basis_weights.shape[0]
    block = jax.ShapeDtypeStruct((ELEMS, NODES, columns), F32)
    edge = jax.ShapeDtypeStruct((16, columns), F32)
    listed = jax.ShapeDtypeStruct((CAP, NODES, columns), F32)
    mats = jax.ShapeDtypeStruct((steps, 256, 256), BF16)
    table = pltpu.SMEM(
        (min(8, send_list.shape[1]), 128 if send_list.shape[2] % 128 == 0 else send_list.shape[2]), jnp.int32
    )
    field = tracers.reshape(ELEMS, NODES, columns)
    weights = basis_weights.reshape(steps, 256, 16)

    sends = pl.pallas_call(
        first_gather, name="first_gather", out_shape=[listed] * 4, in_specs=[HBM, HBM], out_specs=[VMEM] * 4,
        scratch_shapes=[table, pltpu.SemaphoreType.DMA, pltpu.SemaphoreType.DMA((16,))],
        cost_estimate=cost(3 << 20), compiler_params=grant(12),
    )(pltpu.with_memory_space_constraint(send_list, pltpu.HBM), pltpu.with_memory_space_constraint(field, pltpu.HBM))
    high, low = pl.pallas_call(
        spread_weights, name="spread_weights", out_shape=[mats] * 2, in_specs=[VMEM], out_specs=[VMEM] * 2,
        cost_estimate=cost(2 << 20), compiler_params=grant(12),
    )(weights)
    for step in range(steps):
        face = swaps("face", sends[0], sends[1])
        tile = swaps("tile", sends[2], sends[3])
        moved, *rows = pl.pallas_call(
            functools.partial(move, step), name="move", out_shape=[block, edge, edge],
            in_specs=[SMEM, SMEM] + [VMEM] * 7, out_specs=[VMEM] * 3,
            scratch_shapes=[
                pltpu.VMEM((ELEMS, NODES, columns), F32),
                pltpu.VMEM((256, columns), BF16),
                pltpu.VMEM((256, columns), BF16),
            ],
            cost_estimate=cost(6 << 20), compiler_params=grant(12),
        )(up_owner, up_slot, field, *face, *tile, high, low)
        face = swaps("face", *rows)
        inside, left, right = pl.pallas_call(
            average_inside, name="average_inside", out_shape=[block, edge, edge], in_specs=[VMEM],
            out_specs=[VMEM] * 3, scratch_shapes=[pltpu.VMEM((ELEMS, NODES, columns), F32)],
            cost_estimate=cost(3 << 20), compiler_params=grant(12),
        )(moved)
        columns_out = pl.pallas_call(
            finish_columns, name="finish_columns", out_shape=[edge] * 2, in_specs=[VMEM] * 4, out_specs=[VMEM] * 2,
            cost_estimate=cost(1 << 19), compiler_params=grant(12),
        )(left, right, *face)
        tile = swaps("tile", *columns_out)
        inside = pl.pallas_call(
            finish_rows, name="finish_rows", out_shape=block, in_specs=[VMEM] * 3, out_specs=VMEM,
            cost_estimate=cost(1 << 20), compiler_params=grant(12),
        )(inside, *face)
        if step < steps - 1:
            field, *sends = pl.pallas_call(
                functools.partial(finish_field, step), name="finish_field", out_shape=[block] + [listed] * 4,
                in_specs=[HBM] + [VMEM] * 3, out_specs=[VMEM] * 5,
                scratch_shapes=[table, pltpu.SemaphoreType.DMA], cost_estimate=cost(3 << 20), compiler_params=grant(12),
            )(send_list, inside, *tile)
        else:
            field = pl.pallas_call(
                finish_last, name="finish_last", out_shape=block, in_specs=[VMEM] * 3, out_specs=VMEM,
                cost_estimate=cost(3 << 20), compiler_params=grant(12),
            )(inside, *tile)
    return field.reshape(tracers.shape)


def solution(mesh):
    return jax.shard_map(
        local,
        mesh=mesh,
        in_specs=(
            P("face", "tile", None, None),
            P(None, "face", "tile", None, None),
            P(None, "face", "tile"),
            P(None, "face", "tile"),
            P(),
        ),
        out_specs=P("face", "tile", None, None),
        check_vma=False,
    )
```

```python
import functools

import jax
import jax.numpy as jnp
from jax import lax
from jax.experimental import pallas as pl
from jax.experimental.pallas import tpu as pltpu
from jax.sharding import PartitionSpec as P

F32 = jnp.float32
BF16 = jnp.bfloat16
VMEM = pl.BlockSpec(memory_space=pltpu.VMEM)
SMEM = pl.BlockSpec(memory_space=pltpu.SMEM)
HBM = pl.BlockSpec(memory_space=pltpu.HBM)
ELEMS = 16
NODES = 16
CAP = 4


def cost(cycles_bytes):
    return pl.CostEstimate(flops=0, transcendentals=0, bytes_accessed=cycles_bytes)


def grant(mib):
    return pltpu.CompilerParams(vmem_limit_bytes=mib << 20)


def list_copy(step, lists, table, sem):
    rows, cols = table.shape
    row = lax.axis_index("face") * 4
    col = lax.axis_index("tile") * CAP
    row0, col0 = lax.div(row, rows) * rows, lax.div(col, cols) * cols
    copy = pltpu.make_async_copy(
        lists.at[step, pl.ds(pl.multiple_of(row0, rows), rows), pl.ds(pl.multiple_of(col0, cols), cols)],
        table,
        sem,
    )
    return copy, row - row0, col - col0


def directions():
    return odd("face"), 1 - odd("face"), 2 + odd("tile"), 3 - odd("tile")


def first_gather(axis, lists, field, *rest):
    sends, (table, list_sem, sems) = rest[:2], rest[2:]
    copy, row, col = list_copy(0, lists, table, list_sem)
    copy.start()
    copy.wait()
    copies = []
    toward = directions()[:2] if axis == "face" else directions()[2:]
    for k in (1, 0):
        for c in range(CAP):
            copies.append(
                pltpu.make_async_copy(
                    field.at[table[row + toward[k], col + c]], sends[k].at[c], sems.at[k * CAP + c]
                )
            )
            copies[-1].start()
    for copy in copies:
        copy.wait()


def spread_weights(weights, high, low):
    lane = lax.broadcasted_iota(jnp.int32, (16, 256), 1)
    row = lax.broadcasted_iota(jnp.int32, (16, 256), 0)
    spread = jnp.where(lane % 16 == row, 1.0, 0.0).astype(BF16)
    out_row = lax.broadcasted_iota(jnp.int32, (256, 256), 0)
    out_col = lax.broadcasted_iota(jnp.int32, (256, 256), 1)
    own = out_row // 16 == out_col // 16
    for step in range(weights.shape[0]):
        w = weights[step]
        w_high = w.astype(BF16)
        w_low = (w - w_high.astype(F32)).astype(BF16)
        for part, out in ((w_high, high), (w_low, low)):
            wide = jnp.dot(part, spread, preferred_element_type=F32)
            out[step] = jnp.where(own, wide, 0.0).astype(BF16)


def sublane(shape=(8, 1)):
    return lax.broadcasted_iota(jnp.int32, shape, 0)


def roll(x, by):
    return x if by % 8 == 0 else pltpu.roll(x, by % 8, 0)


def move(step, owner, slot, field, face_first, face_second, tile_first, tile_second, high, low,
         moved, row_first, row_second, source, split_high, split_low):
    owners = (2 - odd("face"), 1 + odd("face"), 4 - odd("tile"), 3 + odd("tile"))
    for e in range(ELEMS):
        o = owner[step, e // 4, e % 4]
        p = slot[step, e // 4, e % 4]
        c = jnp.minimum(p, CAP - 1)
        block = field[p]
        for code, arrived in zip(owners, (face_first, face_second, tile_first, tile_second)):
            block = jnp.where(o == code, arrived[c], block)
        source[e] = block
        part = block.astype(BF16)
        split_high[pl.ds(e * 16, 16), :] = part
        split_low[pl.ds(e * 16, 16), :] = (block - part.astype(F32)).astype(BF16)
    wide = 256
    for n in range(0, field.shape[2], wide):
        cols = pl.ds(n, wide)
        s_high, s_low = split_high[:, cols], split_low[:, cols]
        w_high, w_low = high[step], low[step]
        total = jnp.dot(w_high, s_high, preferred_element_type=F32)
        total += jnp.dot(w_high, s_low, preferred_element_type=F32)
        total += jnp.dot(w_low, s_high, preferred_element_type=F32)
        for e in range(ELEMS):
            src = source[e, :, cols]
            least = jnp.min(src, axis=0, keepdims=True)
            most = jnp.max(src, axis=0, keepdims=True)
            moved[e, :, cols] = jnp.clip(total[e * 16 : e * 16 + 16], least, most)
    sub = sublane()
    packed = []
    for x, tile in ((0, 0), (3, 1)):
        rows = []
        for pair in range(2):
            even = moved[4 * x + 2 * pair, 8 * tile : 8 * tile + 8, :]
            after = moved[4 * x + 2 * pair + 1, 8 * tile : 8 * tile + 8, :]
            if tile == 0:
                rows.append(jnp.where(sub < 4, even, roll(after, 4)))
            else:
                rows.append(jnp.where(sub < 4, roll(even, 4), after))
        left, right = rows
        inner = []
        for t in rows:
            t2 = jnp.where(sub == 3, 0.5 * (t + roll(t, 7)), t)
            inner.append(jnp.where(sub == 4, 0.5 * (t + roll(t, 1)), t2))
        inner[0] = jnp.where(sub == 7, 0.5 * (left + roll(right, 7)), inner[0])
        inner[1] = jnp.where(sub == 0, 0.5 * (right + roll(left, 1)), inner[1])
        packed.append(inner)
    flip = odd("face") == 1
    for k in range(2):
        rows = slice(8 * k, 8 * k + 8)
        top, bottom = packed[0][k], packed[1][k]
        row_first[rows, :] = jnp.where(flip, top, bottom)
        row_second[rows, :] = jnp.where(flip, bottom, top)


def average_inside(moved, inside, left, right, draft):
    sub = sublane()
    first, last = sub % 4 == 0, sub % 4 == 3
    for e in range(ELEMS):
        y = e % 4
        for k in range(2):
            rows = slice(8 * k, 8 * k + 8)
            m = moved[e, rows, :]
            c = m
            if y < 3:
                c = jnp.where(last, 0.5 * (m + roll(moved[e + 1, rows, :], 3)), c)
            if y > 0:
                c = jnp.where(first, 0.5 * (m + roll(moved[e - 1, rows, :], 5)), c)
            draft[e, rows, :] = c
    for e in range(ELEMS):
        x = e // 4
        t0, t1 = draft[e, 0:8, :], draft[e, 8:16, :]
        if x > 0:
            t0 = jnp.where(sub < 4, 0.5 * (t0 + roll(draft[e - 4, 8:16, :], 4)), t0)
        if x < 3:
            t1 = jnp.where(sub >= 4, 0.5 * (t1 + roll(draft[e + 4, 0:8, :], 4)), t1)
        inside[e, 0:8, :] = t0
        inside[e, 8:16, :] = t1
    for out, y, at in ((left, 0, 0), (right, 3, 3)):
        for pair in range(2):
            packed = None
            for place in range(4):
                e = 4 * (2 * pair + place // 2) + y
                k = place % 2
                t = roll(inside[e, 8 * k : 8 * k + 8, :], place - at)
                packed = t if packed is None else jnp.where(sub % 4 == place, t, packed)
            out[8 * pair : 8 * pair + 8, :] = packed


def finish_columns(left, right, face_first, face_second, column_first, column_second):
    sub = sublane()
    flip = odd("face") == 1
    lo, hi = slice(0, 8), slice(8, 16)
    a0, a1, b0, b1 = (
        jnp.where(flip == from_first, face_first[rows, :], face_second[rows, :])
        for from_first in (True, False)
        for rows in (lo, hi)
    )
    l0 = jnp.where(sub == 0, 0.5 * (left[lo, :] + a0), left[lo, :])
    l1 = jnp.where(sub == 7, 0.5 * (left[hi, :] + roll(b0, 7)), left[hi, :])
    r0 = jnp.where(sub == 0, 0.5 * (right[lo, :] + roll(a1, 1)), right[lo, :])
    r1 = jnp.where(sub == 7, 0.5 * (right[hi, :] + b1), right[hi, :])
    flip = odd("tile") == 1
    for rows, l, r in ((lo, l0, r0), (hi, l1, r1)):
        column_first[rows, :] = jnp.where(flip, l, r)
        column_second[rows, :] = jnp.where(flip, r, l)


def finish_rows(inside, face_first, face_second, out):
    sub = sublane()
    flip = odd("face") == 1
    out[4:12] = inside[4:12]
    for y in range(4):
        first = face_first[8 * (y // 2) : 8 * (y // 2) + 8, :]
        second = face_second[8 * (y // 2) : 8 * (y // 2) + 8, :]
        a, b = jnp.where(flip, first, second), jnp.where(flip, second, first)
        t = inside[y, 0:8, :]
        out[y, 0:8, :] = jnp.where(sub < 4, 0.5 * (t + roll(a, 4 * (y % 2))), t)
        out[y, 8:16, :] = inside[y, 8:16, :]
        out[12 + y, 0:8, :] = inside[12 + y, 0:8, :]
        t = inside[12 + y, 8:16, :]
        out[12 + y, 8:16, :] = jnp.where(sub >= 4, 0.5 * (t + roll(b, 4 - 4 * (y % 2))), t)


def fix_edges(inside, tile_first, tile_second, out):
    sub = sublane()
    first, last = sub % 4 == 0, sub % 4 == 3
    flip = odd("tile") == 1
    for x in range(4):
        one = tile_first[8 * (x // 2) : 8 * (x // 2) + 8, :]
        two = tile_second[8 * (x // 2) : 8 * (x // 2) + 8, :]
        before, after = jnp.where(flip, one, two), jnp.where(flip, two, one)
        out[4 * x + 1 : 4 * x + 3] = inside[4 * x + 1 : 4 * x + 3]
        for k in range(2):
            place = 2 * (x % 2) + k
            rows = slice(8 * k, 8 * k + 8)
            t = inside[4 * x, rows, :]
            out[4 * x, rows, :] = jnp.where(first, 0.5 * (t + roll(before, -place)), t)
            t = inside[4 * x + 3, rows, :]
            out[4 * x + 3, rows, :] = jnp.where(last, 0.5 * (t + roll(after, 3 - place)), t)


def finish_field(step, lists, inside, tile_first, tile_second, field, *rest):
    sends, (table, list_sem) = rest[:4], rest[4:]
    copy, row, col = list_copy(step + 1, lists, table, list_sem)
    copy.start()
    fix_edges(inside, tile_first, tile_second, field)
    copy.wait()
    for k, j in enumerate(directions()):
        for c in range(CAP):
            sends[k][c] = field[table[row + j, col + c]]


def finish_last(inside, tile_first, tile_second, field):
    fix_edges(inside, tile_first, tile_second, field)


def swap(axis, offset, x):
    count = lax.axis_size(axis)
    pairs = []
    for i in range(offset, count + offset, 2):
        pairs += [(i % count, (i + 1) % count), ((i + 1) % count, i % count)]
    return lax.ppermute(x, axis, sorted(pairs))


def swaps(axis, first, second):
    return swap(axis, 0, first), swap(axis, 1, second)


def odd(axis):
    return lax.rem(lax.axis_index(axis), 2)


def transport(tracers, basis_weights, up_owner, up_slot, send_list):
    columns = tracers.shape[3]
    steps = basis_weights.shape[0]
    block = jax.ShapeDtypeStruct((ELEMS, NODES, columns), F32)
    edge = jax.ShapeDtypeStruct((16, columns), F32)
    listed = jax.ShapeDtypeStruct((CAP, NODES, columns), F32)
    mats = jax.ShapeDtypeStruct((steps, 256, 256), BF16)
    table = pltpu.SMEM(
        (min(8, send_list.shape[1]), 128 if send_list.shape[2] % 128 == 0 else send_list.shape[2]), jnp.int32
    )
    field = tracers.reshape(ELEMS, NODES, columns)
    weights = basis_weights.reshape(steps, 256, 16)

    lists_hbm = pltpu.with_memory_space_constraint(send_list, pltpu.HBM)
    field_hbm = pltpu.with_memory_space_constraint(field, pltpu.HBM)
    sends = []
    for axis in ("face", "tile"):
        sends += pl.pallas_call(
            functools.partial(first_gather, axis), out_shape=[listed] * 2,
            in_specs=[HBM, HBM], out_specs=[VMEM] * 2,
            scratch_shapes=[table, pltpu.SemaphoreType.DMA, pltpu.SemaphoreType.DMA((8,))],
            cost_estimate=cost(2 << 20), compiler_params=grant(12),
        )(lists_hbm, field_hbm)
    high, low = pl.pallas_call(
        spread_weights, name="spread_weights", out_shape=[mats] * 2, in_specs=[VMEM], out_specs=[VMEM] * 2,
        cost_estimate=cost(2 << 20), compiler_params=grant(12),
    )(weights)
    for step in range(steps):
        face = swaps("face", sends[0], sends[1])
        tile = swaps("tile", sends[2], sends[3])
        moved, *rows = pl.pallas_call(
            functools.partial(move, step), name="move", out_shape=[block, edge, edge],
            in_specs=[SMEM, SMEM] + [VMEM] * 7, out_specs=[VMEM] * 3,
            scratch_shapes=[
                pltpu.VMEM((ELEMS, NODES, columns), F32),
                pltpu.VMEM((256, columns), BF16),
                pltpu.VMEM((256, columns), BF16),
            ],
            cost_estimate=cost(6 << 20), compiler_params=grant(12),
        )(up_owner, up_slot, field, *face, *tile, high, low)
        face = swaps("face", *rows)
        inside, left, right = pl.pallas_call(
            average_inside, name="average_inside", out_shape=[block, edge, edge], in_specs=[VMEM],
            out_specs=[VMEM] * 3, scratch_shapes=[pltpu.VMEM((ELEMS, NODES, columns), F32)],
            cost_estimate=cost(3 << 20), compiler_params=grant(12),
        )(moved)
        columns_out = pl.pallas_call(
            finish_columns, name="finish_columns", out_shape=[edge] * 2, in_specs=[VMEM] * 4, out_specs=[VMEM] * 2,
            cost_estimate=cost(1 << 19), compiler_params=grant(12),
        )(left, right, *face)
        tile = swaps("tile", *columns_out)
        inside = pl.pallas_call(
            finish_rows, name="finish_rows", out_shape=block, in_specs=[VMEM] * 3, out_specs=VMEM,
            cost_estimate=cost(1 << 20), compiler_params=grant(12),
        )(inside, *face)
        if step < steps - 1:
            field, *sends = pl.pallas_call(
                functools.partial(finish_field, step), name="finish_field", out_shape=[block] + [listed] * 4,
                in_specs=[HBM] + [VMEM] * 3, out_specs=[VMEM] * 5,
                scratch_shapes=[table, pltpu.SemaphoreType.DMA], cost_estimate=cost(3 << 20), compiler_params=grant(12),
            )(send_list, inside, *tile)
        else:
            field = pl.pallas_call(
                finish_last, name="finish_last", out_shape=block, in_specs=[VMEM] * 3, out_specs=VMEM,
                cost_estimate=cost(3 << 20), compiler_params=grant(12),
            )(inside, *tile)
    return field.reshape(tracers.shape)


def solution(mesh):
    return jax.shard_map(
        transport,
        mesh=mesh,
        in_specs=(
            P("face", "tile", None, None),
            P(None, "face", "tile", None, None),
            P(None, "face", "tile"),
            P(None, "face", "tile"),
            P(),
        ),
        out_specs=P("face", "tile", None, None),
        check_vma=False,
    )
```

```python
import functools

import jax
import jax.numpy as jnp
from jax import lax
from jax.experimental import pallas as pl
from jax.experimental.pallas import tpu as pltpu
from jax.sharding import PartitionSpec as P

F32 = jnp.float32
BF16 = jnp.bfloat16
VMEM = pl.BlockSpec(memory_space=pltpu.VMEM)
SMEM = pl.BlockSpec(memory_space=pltpu.SMEM)
HBM = pl.BlockSpec(memory_space=pltpu.HBM)
ELEMS = 16
NODES = 16
CAP = 4


def run(kernel, in_specs, out, mib, scratch, *args, out_space=VMEM):
    out_specs = [out_space] * len(out) if isinstance(out, list) else out_space
    return pl.pallas_call(
        kernel,
        out_shape=out,
        in_specs=in_specs,
        out_specs=out_specs,
        scratch_shapes=scratch,
        cost_estimate=pl.CostEstimate(flops=0, transcendentals=0, bytes_accessed=mib << 20),
        compiler_params=pltpu.CompilerParams(vmem_limit_bytes=12 << 20),
    )(*args)


def list_copy(step, lists, table, sem):
    rows, cols = table.shape
    row = lax.axis_index("face") * 4
    col = lax.axis_index("tile") * CAP
    row0, col0 = lax.div(row, rows) * rows, lax.div(col, cols) * cols
    copy = pltpu.make_async_copy(
        lists.at[step, pl.ds(pl.multiple_of(row0, rows), rows), pl.ds(pl.multiple_of(col0, cols), cols)],
        table,
        sem,
    )
    return copy, row - row0, col - col0


def directions():
    return odd("face"), 1 - odd("face"), 2 + odd("tile"), 3 - odd("tile")


def first_gather(lists, field, face_first, face_second, tile_first, tile_second, held, table, list_sem, sem):
    copy, row, col = list_copy(0, lists, table, list_sem)
    copy.start()
    whole = pltpu.make_async_copy(field, held, sem)
    whole.start()
    copy.wait()
    whole.wait()
    for send, j in zip((face_first, face_second, tile_first, tile_second), directions()):
        for c in range(CAP):
            send[c] = held[table[row + j, col + c]]


def read_lists(step, lists, listed, table, list_sem):
    copy, row, col = list_copy(step, lists, table, list_sem)
    copy.start()
    copy.wait()
    at_row = lax.broadcasted_iota(jnp.int32, listed.shape, 0)
    at_col = lax.broadcasted_iota(jnp.int32, listed.shape, 1)
    values = jnp.zeros(listed.shape, jnp.int32)
    for k, j in enumerate(directions()):
        for c in range(CAP):
            values = jnp.where((at_row == k) & (at_col == c), table[row + j, col + c], values)
    listed[...] = values


def spread_weights(weights, high, low, joined):
    lane = lax.broadcasted_iota(jnp.int32, (16, 256), 1)
    row = lax.broadcasted_iota(jnp.int32, (16, 256), 0)
    spread = jnp.where(lane % 16 == row, 1.0, 0.0).astype(BF16)
    out_row = lax.broadcasted_iota(jnp.int32, (256, 256), 0)
    out_col = lax.broadcasted_iota(jnp.int32, (256, 256), 1)
    own = out_row // 16 == out_col // 16
    for step in range(weights.shape[0]):
        w = weights[step]
        w_high = w.astype(BF16)
        w_low = (w - w_high.astype(F32)).astype(BF16)
        joined[step] = jnp.concatenate([w_high, w_high, w_low], axis=1).reshape(16, 16, 48)
        for part, out in ((w_high, high), (w_low, low)):
            wide = jnp.dot(part, spread, preferred_element_type=F32)
            out[step] = jnp.where(own, wide, 0.0).astype(BF16)


def sublane(shape=(8, 1)):
    return lax.broadcasted_iota(jnp.int32, shape, 0)


def roll(x, by):
    return x if by % 8 == 0 else pltpu.roll(x, by % 8, 0)


def move_most(step, owner, slot, field, face_first, face_second, tile_first, high, low, joined,
              moved, far_weights, is_far, source, split_high, split_low):
    owners = (2 - odd("face"), 1 + odd("face"), 4 - odd("tile"))
    far = 3 + odd("tile")
    target = [jnp.int32(-1)] * CAP
    for e in range(ELEMS):
        o = owner[step, e // 4, e % 4]
        p = slot[step, e // 4, e % 4]
        c = jnp.minimum(p, CAP - 1)
        block = field[p]
        for code, arrived in zip(owners, (face_first, face_second, tile_first)):
            block = jnp.where(o == code, arrived[c], block)
        for k in range(CAP):
            hit = (o == far) & (p == k)
            target[k] = jnp.where(hit, e, target[k])
            is_far[k * ELEMS + e : k * ELEMS + e + 1, :] = jnp.full((1, 128), jnp.where(hit, 1.0, 0.0), F32)
        source[e] = block
        part = block.astype(BF16)
        split_high[pl.ds(e * 16, 16), :] = part
        split_low[pl.ds(e * 16, 16), :] = (block - part.astype(F32)).astype(BF16)
    for k in range(CAP):
        far_weights[k] = joined[step, jnp.maximum(target[k], 0)]
    wide = 256
    for n in range(0, field.shape[2], wide):
        cols = pl.ds(n, wide)
        s_high, s_low = split_high[:, cols], split_low[:, cols]
        w_high, w_low = high[step], low[step]
        total = jnp.dot(w_high, s_high, preferred_element_type=F32)
        total += jnp.dot(w_high, s_low, preferred_element_type=F32)
        total += jnp.dot(w_low, s_high, preferred_element_type=F32)
        for e in range(ELEMS):
            src = source[e, :, cols]
            least = jnp.min(src, axis=0, keepdims=True)
            most = jnp.max(src, axis=0, keepdims=True)
            moved[e, :, cols] = jnp.clip(total[e * 16 : e * 16 + 16], least, most)


def with_far(e, rows, cols, moved, far, is_far):
    t = moved[e, rows, cols]
    for k in range(CAP):
        t = jnp.where(is_far[k * ELEMS + e : k * ELEMS + e + 1, :] > 0.5, far[k, rows, cols], t)
    return t


def move_far(arrived, far_weights, moved, is_far, far, row_first, row_second):
    for k in range(CAP):
        src = arrived[k]
        s_high = src.astype(BF16)
        s_low = (src - s_high.astype(F32)).astype(BF16)
        total = jnp.dot(
            far_weights[k], jnp.concatenate([s_high, s_low, s_high], axis=0), preferred_element_type=F32
        )
        far[k] = jnp.clip(total, jnp.min(src, axis=0, keepdims=True), jnp.max(src, axis=0, keepdims=True))
    sub = sublane()
    flip = odd("face") == 1
    for n in range(0, moved.shape[2], 128):
        cols = slice(n, n + 128)
        packed = []
        for x, tile in ((0, 0), (3, 1)):
            rows = []
            for pair in range(2):
                at = slice(8 * tile, 8 * tile + 8)
                even = with_far(4 * x + 2 * pair, at, cols, moved, far, is_far)
                after = with_far(4 * x + 2 * pair + 1, at, cols, moved, far, is_far)
                if tile == 0:
                    rows.append(jnp.where(sub < 4, even, roll(after, 4)))
                else:
                    rows.append(jnp.where(sub < 4, roll(even, 4), after))
            left, right = rows
            inner = []
            for t in rows:
                t2 = jnp.where(sub == 3, 0.5 * (t + roll(t, 7)), t)
                inner.append(jnp.where(sub == 4, 0.5 * (t + roll(t, 1)), t2))
            inner[0] = jnp.where(sub == 7, 0.5 * (left + roll(right, 7)), inner[0])
            inner[1] = jnp.where(sub == 0, 0.5 * (right + roll(left, 1)), inner[1])
            packed.append(inner)
        for k in range(2):
            rows = slice(8 * k, 8 * k + 8)
            top, bottom = packed[0][k], packed[1][k]
            row_first[rows, cols] = jnp.where(flip, top, bottom)
            row_second[rows, cols] = jnp.where(flip, bottom, top)


def average_inside(moved, far, is_far, inside, left, right, draft, whole):
    sub = sublane()
    for e in range(ELEMS):
        for k in range(2):
            rows = slice(8 * k, 8 * k + 8)
            for n in range(0, moved.shape[2], 128):
                cols = slice(n, n + 128)
                whole[e, rows, cols] = with_far(e, rows, cols, moved, far, is_far)
    moved = whole
    first, last = sub % 4 == 0, sub % 4 == 3
    for e in range(ELEMS):
        y = e % 4
        for k in range(2):
            rows = slice(8 * k, 8 * k + 8)
            m = moved[e, rows, :]
            c = m
            if y < 3:
                c = jnp.where(last, 0.5 * (m + roll(moved[e + 1, rows, :], 3)), c)
            if y > 0:
                c = jnp.where(first, 0.5 * (m + roll(moved[e - 1, rows, :], 5)), c)
            draft[e, rows, :] = c
    for e in range(ELEMS):
        x = e // 4
        t0, t1 = draft[e, 0:8, :], draft[e, 8:16, :]
        if x > 0:
            t0 = jnp.where(sub < 4, 0.5 * (t0 + roll(draft[e - 4, 8:16, :], 4)), t0)
        if x < 3:
            t1 = jnp.where(sub >= 4, 0.5 * (t1 + roll(draft[e + 4, 0:8, :], 4)), t1)
        inside[e, 0:8, :] = t0
        inside[e, 8:16, :] = t1
    for out, y, at in ((left, 0, 0), (right, 3, 3)):
        for pair in range(2):
            packed = None
            for place in range(4):
                e = 4 * (2 * pair + place // 2) + y
                k = place % 2
                t = roll(inside[e, 8 * k : 8 * k + 8, :], place - at)
                packed = t if packed is None else jnp.where(sub % 4 == place, t, packed)
            out[8 * pair : 8 * pair + 8, :] = packed


def finish_columns(left, right, face_first, face_second, column_first, column_second):
    sub = sublane()
    flip = odd("face") == 1
    lo, hi = slice(0, 8), slice(8, 16)
    a0, a1, b0, b1 = (
        jnp.where(flip == from_first, face_first[rows, :], face_second[rows, :])
        for from_first in (True, False)
        for rows in (lo, hi)
    )
    l0 = jnp.where(sub == 0, 0.5 * (left[lo, :] + a0), left[lo, :])
    l1 = jnp.where(sub == 7, 0.5 * (left[hi, :] + roll(b0, 7)), left[hi, :])
    r0 = jnp.where(sub == 0, 0.5 * (right[lo, :] + roll(a1, 1)), right[lo, :])
    r1 = jnp.where(sub == 7, 0.5 * (right[hi, :] + b1), right[hi, :])
    flip = odd("tile") == 1
    for rows, l, r in ((lo, l0, r0), (hi, l1, r1)):
        column_first[rows, :] = jnp.where(flip, l, r)
        column_second[rows, :] = jnp.where(flip, r, l)


def finish_rows(inside, face_first, face_second, out):
    sub = sublane()
    flip = odd("face") == 1
    out[4:12] = inside[4:12]
    for y in range(4):
        first = face_first[8 * (y // 2) : 8 * (y // 2) + 8, :]
        second = face_second[8 * (y // 2) : 8 * (y // 2) + 8, :]
        a, b = jnp.where(flip, first, second), jnp.where(flip, second, first)
        t = inside[y, 0:8, :]
        out[y, 0:8, :] = jnp.where(sub < 4, 0.5 * (t + roll(a, 4 * (y % 2))), t)
        out[y, 8:16, :] = inside[y, 8:16, :]
        out[12 + y, 0:8, :] = inside[12 + y, 0:8, :]
        t = inside[12 + y, 8:16, :]
        out[12 + y, 8:16, :] = jnp.where(sub >= 4, 0.5 * (t + roll(b, 4 - 4 * (y % 2))), t)


def fix_edges(inside, tile_first, tile_second, put):
    sub = sublane()
    first, last = sub % 4 == 0, sub % 4 == 3
    flip = odd("tile") == 1
    for x in range(4):
        one = tile_first[8 * (x // 2) : 8 * (x // 2) + 8, :]
        two = tile_second[8 * (x // 2) : 8 * (x // 2) + 8, :]
        before, after = jnp.where(flip, one, two), jnp.where(flip, two, one)
        for k in range(2):
            place = 2 * (x % 2) + k
            rows = slice(8 * k, 8 * k + 8)
            t = inside[4 * x, rows, :]
            put(x, 0, rows, jnp.where(first, 0.5 * (t + roll(before, -place)), t))
            t = inside[4 * x + 3, rows, :]
            put(x, 1, rows, jnp.where(last, 0.5 * (t + roll(after, 3 - place)), t))


def finish_sends(listed, inside, tile_first, tile_second, *rest):
    sends, edges = rest[:4], rest[4]
    values = listed[...]

    def put(x, right, rows, t):
        edges[2 * x + right, rows, :] = t

    fix_edges(inside, tile_first, tile_second, put)
    for k in range(4):
        for c in range(CAP):
            e = values[k, c]
            y = e & 3
            at_edge = (y == 0) | (y == 3)
            place = 2 * (e >> 2) + (y >> 1)
            sends[k][c] = jnp.where(at_edge, edges[place], inside[e])


def finish_field(inside, tile_first, tile_second, field):
    def put(x, right, rows, t):
        field[4 * x + 3 * right, rows, :] = t

    fix_edges(inside, tile_first, tile_second, put)
    for x in range(4):
        field[4 * x + 1 : 4 * x + 3] = inside[4 * x + 1 : 4 * x + 3]


def finish_last(inside, tile_first, tile_second, field, edges, sems):
    copies = []
    for x in range(4):
        part = pl.ds(4 * x + 1, 2)
        copies.append(pltpu.make_async_copy(inside.at[part], field.at[part], sems.at[x]))
        copies[-1].start()

    def put(x, right, rows, t):
        edges[2 * x + right, rows, :] = t

    fix_edges(inside, tile_first, tile_second, put)
    for i in range(8):
        copies.append(
            pltpu.make_async_copy(edges.at[i], field.at[4 * (i // 2) + 3 * (i % 2)], sems.at[4 + i])
        )
        copies[-1].start()
    for copy in copies:
        copy.wait()


def swap(axis, offset, x):
    count = lax.axis_size(axis)
    pairs = []
    for i in range(offset, count + offset, 2):
        pairs += [(i % count, (i + 1) % count), ((i + 1) % count, i % count)]
    return lax.ppermute(x, axis, sorted(pairs))


def swaps(axis, first, second):
    return swap(axis, 0, first), swap(axis, 1, second)


def odd(axis):
    return lax.rem(lax.axis_index(axis), 2)


def transport(tracers, basis_weights, up_owner, up_slot, send_list):
    columns = tracers.shape[3]
    steps = basis_weights.shape[0]
    block = jax.ShapeDtypeStruct((ELEMS, NODES, columns), F32)
    edge = jax.ShapeDtypeStruct((16, columns), F32)
    listed = jax.ShapeDtypeStruct((CAP, NODES, columns), F32)
    mats = jax.ShapeDtypeStruct((steps, 256, 256), BF16)
    own = jax.ShapeDtypeStruct((steps, 16, 16, 48), BF16)
    far_own = jax.ShapeDtypeStruct((CAP, 16, 48), BF16)
    own_lists = jax.ShapeDtypeStruct((8, 128), jnp.int32)
    flags = jax.ShapeDtypeStruct((CAP * ELEMS, 128), F32)
    table = pltpu.SMEM(
        (min(8, send_list.shape[1]), 128 if send_list.shape[2] % 128 == 0 else send_list.shape[2]), jnp.int32
    )
    field = tracers.reshape(ELEMS, NODES, columns)
    weights = basis_weights.reshape(steps, 256, 16)

    lists_hbm = pltpu.with_memory_space_constraint(send_list, pltpu.HBM)
    field_hbm = pltpu.with_memory_space_constraint(field, pltpu.HBM)
    whole = pltpu.VMEM(block.shape, F32)
    edges = pltpu.VMEM((8, NODES, columns), F32)
    halves = pltpu.VMEM((256, columns), BF16)
    dma = pltpu.SemaphoreType.DMA
    *sends, field = run(first_gather, [HBM, HBM], [listed] * 4 + [block], 1, [table, dma, dma], lists_hbm, field_hbm)
    high, low, joined = run(spread_weights, [VMEM], [mats, mats, own], 1, [], weights)
    for step in range(steps):
        face = swaps("face", sends[0], sends[1])
        tile = swaps("tile", sends[2], sends[3])
        if step < steps - 1:
            upcoming = run(functools.partial(read_lists, step + 1), [HBM], own_lists, 1, [table, dma], lists_hbm)
        if step > 0:
            field = run(finish_field, [VMEM] * 3, block, 2, [], inside, *edge_tile)
        moved, far_weights, is_far = run(
            functools.partial(move_most, step), [SMEM, SMEM] + [VMEM] * 7,
            [block, far_own, flags], 5, [whole, halves, halves],
            up_owner, up_slot, field, *face, tile[0], high, low, joined,
        )
        far, *rows = run(move_far, [VMEM] * 4, [listed, edge, edge], 1, [], tile[1], far_weights, moved, is_far)
        edge_face = swaps("face", *rows)
        inside, left, right = run(
            average_inside, [VMEM] * 3, [block, edge, edge], 3, [whole, whole],
            moved, far, is_far,
        )
        ends = run(finish_columns, [VMEM] * 4, [edge] * 2, 1, [], left, right, *edge_face)
        edge_tile = swaps("tile", *ends)
        inside = run(finish_rows, [VMEM] * 3, block, 1, [], inside, *edge_face)
        if step < steps - 1:
            sends = run(finish_sends, [VMEM] * 4, [listed] * 4, 2, [edges], upcoming, inside, *edge_tile)
        else:
            field = run(
                finish_last, [VMEM] * 3, block, 2, [edges, dma((12,))], inside, *edge_tile,
                out_space=HBM,
            )
    return field.reshape(tracers.shape)


def solution(mesh):
    return jax.shard_map(
        transport,
        mesh=mesh,
        in_specs=(
            P("face", "tile", None, None),
            P(None, "face", "tile", None, None),
            P(None, "face", "tile"),
            P(None, "face", "tile"),
            P(),
        ),
        out_specs=P("face", "tile", None, None),
        check_vma=False,
    )
```

```python
import functools

import jax
import jax.numpy as jnp
from jax import lax
from jax.experimental import pallas as pl
from jax.experimental.pallas import tpu as pltpu
from jax.sharding import PartitionSpec as P

F32 = jnp.float32
BF16 = jnp.bfloat16
VMEM = pl.BlockSpec(memory_space=pltpu.VMEM)
SMEM = pl.BlockSpec(memory_space=pltpu.SMEM)
HBM = pl.BlockSpec(memory_space=pltpu.HBM)
LAST = 0
ELEMS = 16
NODES = 16
CAP = 4


def run(kernel, in_specs, out, mib, scratch, *args, out_space=VMEM):
    out_specs = [out_space] * len(out) if isinstance(out, list) else out_space
    return pl.pallas_call(
        kernel,
        out_shape=out,
        in_specs=in_specs,
        out_specs=out_specs,
        scratch_shapes=scratch,
        cost_estimate=pl.CostEstimate(flops=0, transcendentals=0, bytes_accessed=mib << 20),
        compiler_params=pltpu.CompilerParams(vmem_limit_bytes=12 << 20),
    )(*args)


def list_copy(step, lists, table, sem):
    rows, cols = table.shape
    row = lax.axis_index("face") * 4
    col = lax.axis_index("tile") * CAP
    row0, col0 = lax.div(row, rows) * rows, lax.div(col, cols) * cols
    copy = pltpu.make_async_copy(
        lists.at[step, pl.ds(pl.multiple_of(row0, rows), rows), pl.ds(pl.multiple_of(col0, cols), cols)],
        table,
        sem,
    )
    return copy, row - row0, col - col0


def directions():
    return odd("mixed"), 1 - odd("mixed"), 2 + odd("tile"), 3 - odd("tile")


def first_gather(lists, field, face_first, face_second, tile_first, tile_second, held, table, list_sem, sem):
    copy, row, col = list_copy(0, lists, table, list_sem)
    copy.start()
    whole = pltpu.make_async_copy(field, held, sem)
    whole.start()
    copy.wait()
    whole.wait()
    for send, j in zip((face_first, face_second, tile_first, tile_second), directions()):
        for c in range(CAP):
            send[c] = held[table[row + j, col + c]]


def read_lists(step, lists, listed, table, list_sem):
    copy, row, col = list_copy(step, lists, table, list_sem)
    copy.start()
    copy.wait()
    at_row = lax.broadcasted_iota(jnp.int32, listed.shape, 0)
    at_col = lax.broadcasted_iota(jnp.int32, listed.shape, 1)
    values = jnp.zeros(listed.shape, jnp.int32)
    for k, j in enumerate(directions()):
        for c in range(CAP):
            values = jnp.where((at_row == k) & (at_col == c), table[row + j, col + c], values)
    listed[...] = values


def spread_weights(weights, high, low, joined):
    lane = lax.broadcasted_iota(jnp.int32, (16, 256), 1)
    row = lax.broadcasted_iota(jnp.int32, (16, 256), 0)
    spread = jnp.where(lane % 16 == row, 1.0, 0.0).astype(BF16)
    out_row = lax.broadcasted_iota(jnp.int32, (256, 256), 0)
    out_col = lax.broadcasted_iota(jnp.int32, (256, 256), 1)
    own = out_row // 16 == out_col // 16
    for step in range(weights.shape[0]):
        w = weights[step]
        w_high = w.astype(BF16)
        w_low = (w - w_high.astype(F32)).astype(BF16)
        joined[step] = jnp.concatenate([w_high, w_high, w_low], axis=1).reshape(16, 16, 48)
        for part, out in ((w_high, high), (w_low, low)):
            wide = jnp.dot(part, spread, preferred_element_type=F32)
            out[step] = jnp.where(own, wide, 0.0).astype(BF16)


def sublane(shape=(8, 1)):
    return lax.broadcasted_iota(jnp.int32, shape, 0)


def roll(x, by):
    return x if by % 8 == 0 else pltpu.roll(x, by % 8, 0)


def move_most(step, owner, slot, field, early_a, early_b, early_c, high, low, joined,
              moved, far_weights, is_far, source, split_high, split_low):
    owners = [2 - odd("mixed"), 1 + odd("mixed"), 4 - odd("tile"), 3 + odd("tile")]
    far = owners.pop(LAST)
    target = [jnp.int32(-1)] * CAP
    for e in range(ELEMS):
        o = owner[step, e // 4, e % 4]
        p = slot[step, e // 4, e % 4]
        c = jnp.minimum(p, CAP - 1)
        block = field[p]
        for code, arrived in zip(owners, (early_a, early_b, early_c)):
            block = jnp.where(o == code, arrived[c], block)
        for k in range(CAP):
            hit = (o == far) & (p == k)
            target[k] = jnp.where(hit, e, target[k])
            is_far[k * ELEMS + e : k * ELEMS + e + 1, :] = jnp.full((1, 128), jnp.where(hit, 1.0, 0.0), F32)
        source[e] = block
        part = block.astype(BF16)
        split_high[pl.ds(e * 16, 16), :] = part
        split_low[pl.ds(e * 16, 16), :] = (block - part.astype(F32)).astype(BF16)
    for k in range(CAP):
        far_weights[k] = joined[step, jnp.maximum(target[k], 0)]
    wide = 256
    for n in range(0, field.shape[2], wide):
        cols = pl.ds(n, wide)
        s_high, s_low = split_high[:, cols], split_low[:, cols]
        w_high, w_low = high[step], low[step]
        total = jnp.dot(w_high, s_high, preferred_element_type=F32)
        total += jnp.dot(w_high, s_low, preferred_element_type=F32)
        total += jnp.dot(w_low, s_high, preferred_element_type=F32)
        for e in range(ELEMS):
            src = source[e, :, cols]
            least = jnp.min(src, axis=0, keepdims=True)
            most = jnp.max(src, axis=0, keepdims=True)
            moved[e, :, cols] = jnp.clip(total[e * 16 : e * 16 + 16], least, most)


def with_far(e, rows, cols, moved, far, is_far):
    t = moved[e, rows, cols]
    for k in range(CAP):
        t = jnp.where(is_far[k * ELEMS + e : k * ELEMS + e + 1, :] > 0.5, far[k, rows, cols], t)
    return t


def move_far(arrived, far_weights, moved, is_far, far, row_first, row_second):
    for k in range(CAP):
        src = arrived[k]
        s_high = src.astype(BF16)
        s_low = (src - s_high.astype(F32)).astype(BF16)
        total = jnp.dot(
            far_weights[k], jnp.concatenate([s_high, s_low, s_high], axis=0), preferred_element_type=F32
        )
        far[k] = jnp.clip(total, jnp.min(src, axis=0, keepdims=True), jnp.max(src, axis=0, keepdims=True))
    sub = sublane()
    flip = odd("face") == 1
    for n in range(0, moved.shape[2], 128):
        cols = slice(n, n + 128)
        packed = []
        for x, tile in ((0, 0), (3, 1)):
            rows = []
            for pair in range(2):
                at = slice(8 * tile, 8 * tile + 8)
                even = with_far(4 * x + 2 * pair, at, cols, moved, far, is_far)
                after = with_far(4 * x + 2 * pair + 1, at, cols, moved, far, is_far)
                if tile == 0:
                    rows.append(jnp.where(sub < 4, even, roll(after, 4)))
                else:
                    rows.append(jnp.where(sub < 4, roll(even, 4), after))
            left, right = rows
            inner = []
            for t in rows:
                t2 = jnp.where(sub == 3, 0.5 * (t + roll(t, 7)), t)
                inner.append(jnp.where(sub == 4, 0.5 * (t + roll(t, 1)), t2))
            inner[0] = jnp.where(sub == 7, 0.5 * (left + roll(right, 7)), inner[0])
            inner[1] = jnp.where(sub == 0, 0.5 * (right + roll(left, 1)), inner[1])
            packed.append(inner)
        for k in range(2):
            rows = slice(8 * k, 8 * k + 8)
            top, bottom = packed[0][k], packed[1][k]
            row_first[rows, cols] = jnp.where(flip, top, bottom)
            row_second[rows, cols] = jnp.where(flip, bottom, top)


def average_inside(moved, far, is_far, inside, left, right, draft, whole):
    sub = sublane()
    for e in range(ELEMS):
        for k in range(2):
            rows = slice(8 * k, 8 * k + 8)
            for n in range(0, moved.shape[2], 128):
                cols = slice(n, n + 128)
                whole[e, rows, cols] = with_far(e, rows, cols, moved, far, is_far)
    moved = whole
    first, last = sub % 4 == 0, sub % 4 == 3
    for e in range(ELEMS):
        y = e % 4
        for k in range(2):
            rows = slice(8 * k, 8 * k + 8)
            m = moved[e, rows, :]
            c = m
            if y < 3:
                c = jnp.where(last, 0.5 * (m + roll(moved[e + 1, rows, :], 3)), c)
            if y > 0:
                c = jnp.where(first, 0.5 * (m + roll(moved[e - 1, rows, :], 5)), c)
            draft[e, rows, :] = c
    for e in range(ELEMS):
        x = e // 4
        t0, t1 = draft[e, 0:8, :], draft[e, 8:16, :]
        if x > 0:
            t0 = jnp.where(sub < 4, 0.5 * (t0 + roll(draft[e - 4, 8:16, :], 4)), t0)
        if x < 3:
            t1 = jnp.where(sub >= 4, 0.5 * (t1 + roll(draft[e + 4, 0:8, :], 4)), t1)
        inside[e, 0:8, :] = t0
        inside[e, 8:16, :] = t1
    for out, y, at in ((left, 0, 0), (right, 3, 3)):
        for pair in range(2):
            packed = None
            for place in range(4):
                e = 4 * (2 * pair + place // 2) + y
                k = place % 2
                t = roll(inside[e, 8 * k : 8 * k + 8, :], place - at)
                packed = t if packed is None else jnp.where(sub % 4 == place, t, packed)
            out[8 * pair : 8 * pair + 8, :] = packed


def finish_columns(left, right, face_first, face_second, column_first, column_second):
    sub = sublane()
    flip = odd("face") == 1
    lo, hi = slice(0, 8), slice(8, 16)
    a0, a1, b0, b1 = (
        jnp.where(flip == from_first, face_first[rows, :], face_second[rows, :])
        for from_first in (True, False)
        for rows in (lo, hi)
    )
    l0 = jnp.where(sub == 0, 0.5 * (left[lo, :] + a0), left[lo, :])
    l1 = jnp.where(sub == 7, 0.5 * (left[hi, :] + roll(b0, 7)), left[hi, :])
    r0 = jnp.where(sub == 0, 0.5 * (right[lo, :] + roll(a1, 1)), right[lo, :])
    r1 = jnp.where(sub == 7, 0.5 * (right[hi, :] + b1), right[hi, :])
    flip = odd("tile") == 1
    for rows, l, r in ((lo, l0, r0), (hi, l1, r1)):
        column_first[rows, :] = jnp.where(flip, l, r)
        column_second[rows, :] = jnp.where(flip, r, l)


def finish_rows(inside, face_first, face_second, out):
    sub = sublane()
    flip = odd("face") == 1
    out[4:12] = inside[4:12]
    for y in range(4):
        first = face_first[8 * (y // 2) : 8 * (y // 2) + 8, :]
        second = face_second[8 * (y // 2) : 8 * (y // 2) + 8, :]
        a, b = jnp.where(flip, first, second), jnp.where(flip, second, first)
        t = inside[y, 0:8, :]
        out[y, 0:8, :] = jnp.where(sub < 4, 0.5 * (t + roll(a, 4 * (y % 2))), t)
        out[y, 8:16, :] = inside[y, 8:16, :]
        out[12 + y, 0:8, :] = inside[12 + y, 0:8, :]
        t = inside[12 + y, 8:16, :]
        out[12 + y, 8:16, :] = jnp.where(sub >= 4, 0.5 * (t + roll(b, 4 - 4 * (y % 2))), t)


def fix_edges(inside, tile_first, tile_second, put):
    sub = sublane()
    first, last = sub % 4 == 0, sub % 4 == 3
    flip = odd("tile") == 1
    for x in range(4):
        one = tile_first[8 * (x // 2) : 8 * (x // 2) + 8, :]
        two = tile_second[8 * (x // 2) : 8 * (x // 2) + 8, :]
        before, after = jnp.where(flip, one, two), jnp.where(flip, two, one)
        for k in range(2):
            place = 2 * (x % 2) + k
            rows = slice(8 * k, 8 * k + 8)
            t = inside[4 * x, rows, :]
            put(x, 0, rows, jnp.where(first, 0.5 * (t + roll(before, -place)), t))
            t = inside[4 * x + 3, rows, :]
            put(x, 1, rows, jnp.where(last, 0.5 * (t + roll(after, 3 - place)), t))


def finish_sends(listed, inside, tile_first, tile_second, *rest):
    sends, edges = rest[:4], rest[4]
    values = listed[...]

    def put(x, right, rows, t):
        edges[2 * x + right, rows, :] = t

    fix_edges(inside, tile_first, tile_second, put)
    for k in range(4):
        for c in range(CAP):
            e = values[k, c]
            y = e & 3
            at_edge = (y == 0) | (y == 3)
            place = 2 * (e >> 2) + (y >> 1)
            sends[k][c] = jnp.where(at_edge, edges[place], inside[e])


def finish_field(inside, tile_first, tile_second, field):
    def put(x, right, rows, t):
        field[4 * x + 3 * right, rows, :] = t

    fix_edges(inside, tile_first, tile_second, put)
    for x in range(4):
        field[4 * x + 1 : 4 * x + 3] = inside[4 * x + 1 : 4 * x + 3]


def finish_last(inside, tile_first, tile_second, field, edges, sems):
    copies = []
    for x in range(4):
        part = pl.ds(4 * x + 1, 2)
        copies.append(pltpu.make_async_copy(inside.at[part], field.at[part], sems.at[x]))
        copies[-1].start()

    def put(x, right, rows, t):
        edges[2 * x + right, rows, :] = t

    fix_edges(inside, tile_first, tile_second, put)
    for i in range(8):
        copies.append(
            pltpu.make_async_copy(edges.at[i], field.at[4 * (i // 2) + 3 * (i % 2)], sems.at[4 + i])
        )
        copies[-1].start()
    for copy in copies:
        copy.wait()


def swap(axis, slot, x):
    faces, tiles = lax.axis_size("face"), lax.axis_size("tile")
    pairs = []
    for f in range(faces):
        for t in range(tiles):
            parity = {"face": f, "mixed": f + t, "tile": t}[axis]
            step = 1 if (parity + slot) % 2 == 0 else -1
            target = f * tiles + (t + step) % tiles if axis == "tile" else (f + step) % faces * tiles + t
            pairs.append((f * tiles + t, target))
    return lax.ppermute(x, ("face", "tile"), pairs)


def swaps(axis, first, second):
    return swap(axis, 0, first), swap(axis, 1, second)


def odd(axis):
    place = lax.axis_index("face" if axis == "face" else "tile")
    if axis == "mixed":
        place += lax.axis_index("face")
    return lax.rem(place, 2)


def transport(tracers, basis_weights, up_owner, up_slot, send_list):
    columns = tracers.shape[3]
    steps = basis_weights.shape[0]
    block = jax.ShapeDtypeStruct((ELEMS, NODES, columns), F32)
    edge = jax.ShapeDtypeStruct((16, columns), F32)
    listed = jax.ShapeDtypeStruct((CAP, NODES, columns), F32)
    mats = jax.ShapeDtypeStruct((steps, 256, 256), BF16)
    own = jax.ShapeDtypeStruct((steps, 16, 16, 48), BF16)
    far_own = jax.ShapeDtypeStruct((CAP, 16, 48), BF16)
    own_lists = jax.ShapeDtypeStruct((8, 128), jnp.int32)
    flags = jax.ShapeDtypeStruct((CAP * ELEMS, 128), F32)
    table = pltpu.SMEM(
        (min(8, send_list.shape[1]), 128 if send_list.shape[2] % 128 == 0 else send_list.shape[2]), jnp.int32
    )
    field = tracers.reshape(ELEMS, NODES, columns)
    weights = basis_weights.reshape(steps, 256, 16)

    lists_hbm = pltpu.with_memory_space_constraint(send_list, pltpu.HBM)
    field_hbm = pltpu.with_memory_space_constraint(field, pltpu.HBM)
    whole = pltpu.VMEM(block.shape, F32)
    edges = pltpu.VMEM((8, NODES, columns), F32)
    halves = pltpu.VMEM((256, columns), BF16)
    dma = pltpu.SemaphoreType.DMA
    *sends, field = run(first_gather, [HBM, HBM], [listed] * 4 + [block], 1, [table, dma, dma], lists_hbm, field_hbm)
    high, low, joined = run(spread_weights, [VMEM], [mats, mats, own], 1, [], weights)
    for step in range(steps):
        face = swaps("mixed", sends[0], sends[1])
        tile = swaps("tile", sends[2], sends[3])
        if step < steps - 1:
            upcoming = run(functools.partial(read_lists, step + 1), [HBM], own_lists, 1, [table, dma], lists_hbm)
        if step > 0:
            field = run(finish_field, [VMEM] * 3, block, 2, [], inside, *edge_tile)
        blocks = [*face, *tile]
        last = blocks.pop(LAST)
        moved, far_weights, is_far = run(
            functools.partial(move_most, step), [SMEM, SMEM] + [VMEM] * 7,
            [block, far_own, flags], 5, [whole, halves, halves],
            up_owner, up_slot, field, *blocks, high, low, joined,
        )
        far, *rows = run(move_far, [VMEM] * 4, [listed, edge, edge], 1, [], last, far_weights, moved, is_far)
        edge_face = swaps("face", *rows)
        inside, left, right = run(
            average_inside, [VMEM] * 3, [block, edge, edge], 3, [whole, whole],
            moved, far, is_far,
        )
        ends = run(finish_columns, [VMEM] * 4, [edge] * 2, 1, [], left, right, *edge_face)
        edge_tile = swaps("tile", *ends)
        inside = run(finish_rows, [VMEM] * 3, block, 1, [], inside, *edge_face)
        if step < steps - 1:
            sends = run(finish_sends, [VMEM] * 4, [listed] * 4, 2, [edges], upcoming, inside, *edge_tile)
        else:
            field = run(
                finish_last, [VMEM] * 3, block, 2, [edges, dma((12,))], inside, *edge_tile,
                out_space=HBM,
            )
    return field.reshape(tracers.shape)


def solution(mesh):
    return jax.shard_map(
        transport,
        mesh=mesh,
        in_specs=(
            P("face", "tile", None, None),
            P(None, "face", "tile", None, None),
            P(None, "face", "tile"),
            P(None, "face", "tile"),
            P(),
        ),
        out_specs=P("face", "tile", None, None),
        check_vma=False,
    )
```

```python
import functools

import jax
import jax.numpy as jnp
from jax import lax
from jax.experimental import pallas as pl
from jax.experimental.pallas import tpu as pltpu
from jax.sharding import PartitionSpec as P

F32 = jnp.float32
BF16 = jnp.bfloat16
VMEM = pl.BlockSpec(memory_space=pltpu.VMEM)
SMEM = pl.BlockSpec(memory_space=pltpu.SMEM)
HBM = pl.BlockSpec(memory_space=pltpu.HBM)
LAST = 0
ELEMS = 16
NODES = 16
CAP = 4


def run(kernel, in_specs, out, mib, scratch, *args, out_space=VMEM):
    out_specs = [out_space] * len(out) if isinstance(out, list) else out_space
    return pl.pallas_call(
        kernel,
        out_shape=out,
        in_specs=in_specs,
        out_specs=out_specs,
        scratch_shapes=scratch,
        cost_estimate=pl.CostEstimate(flops=0, transcendentals=0, bytes_accessed=mib << 20),
        compiler_params=pltpu.CompilerParams(vmem_limit_bytes=12 << 20),
    )(*args)


def list_copy(step, lists, table, sem):
    rows, cols = table.shape
    row = lax.axis_index("face") * 4
    col = lax.axis_index("tile") * CAP
    row0, col0 = lax.div(row, rows) * rows, lax.div(col, cols) * cols
    copy = pltpu.make_async_copy(
        lists.at[step, pl.ds(pl.multiple_of(row0, rows), rows), pl.ds(pl.multiple_of(col0, cols), cols)],
        table,
        sem,
    )
    return copy, row - row0, col - col0


def directions():
    return odd("face"), 1 - odd("face"), 2 + odd("tile"), 3 - odd("tile")


def first_gather(lists, field, face_first, face_second, tile_first, tile_second, held, table, list_sem, sem):
    copy, row, col = list_copy(0, lists, table, list_sem)
    copy.start()
    whole = pltpu.make_async_copy(field, held, sem)
    whole.start()
    copy.wait()
    whole.wait()
    for send, j in zip((face_first, face_second, tile_first, tile_second), directions()):
        for c in range(CAP):
            send[c] = held[table[row + j, col + c]]


def read_lists(step, lists, listed, table, list_sem):
    copy, row, col = list_copy(step, lists, table, list_sem)
    copy.start()
    copy.wait()
    at_row = lax.broadcasted_iota(jnp.int32, listed.shape, 0)
    at_col = lax.broadcasted_iota(jnp.int32, listed.shape, 1)
    values = jnp.zeros(listed.shape, jnp.int32)
    for k, j in enumerate(directions()):
        for c in range(CAP):
            values = jnp.where((at_row == k) & (at_col == c), table[row + j, col + c], values)
    listed[...] = values


def spread_weights(weights, high, low, joined):
    lane = lax.broadcasted_iota(jnp.int32, (16, 256), 1)
    row = lax.broadcasted_iota(jnp.int32, (16, 256), 0)
    spread = jnp.where(lane % 16 == row, 1.0, 0.0).astype(BF16)
    out_row = lax.broadcasted_iota(jnp.int32, (256, 256), 0)
    out_col = lax.broadcasted_iota(jnp.int32, (256, 256), 1)
    own = out_row // 16 == out_col // 16
    for step in range(weights.shape[0]):
        w = weights[step]
        w_high = w.astype(BF16)
        w_low = (w - w_high.astype(F32)).astype(BF16)
        joined[step] = jnp.concatenate([w_high, w_high, w_low], axis=1).reshape(16, 16, 48)
        for part, out in ((w_high, high), (w_low, low)):
            wide = jnp.dot(part, spread, preferred_element_type=F32)
            out[step] = jnp.where(own, wide, 0.0).astype(BF16)


def sublane(shape=(8, 1)):
    return lax.broadcasted_iota(jnp.int32, shape, 0)


def roll(x, by):
    return x if by % 8 == 0 else pltpu.roll(x, by % 8, 0)


def move_most(step, owner, slot, field, early_a, early_b, early_c, high, low, joined,
              moved, far_weights, is_far, source, split_high, split_low):
    owners = [2 - odd("face"), 1 + odd("face"), 4 - odd("tile"), 3 + odd("tile")]
    far = owners.pop(LAST)
    target = [jnp.int32(-1)] * CAP
    for e in range(ELEMS):
        o = owner[step, e // 4, e % 4]
        p = slot[step, e // 4, e % 4]
        c = jnp.minimum(p, CAP - 1)
        block = field[p]
        for code, arrived in zip(owners, (early_a, early_b, early_c)):
            block = jnp.where(o == code, arrived[c], block)
        for k in range(CAP):
            hit = (o == far) & (p == k)
            target[k] = jnp.where(hit, e, target[k])
            is_far[k * ELEMS + e : k * ELEMS + e + 1, :] = jnp.full((1, 128), jnp.where(hit, 1.0, 0.0), F32)
        source[e] = block
        part = block.astype(BF16)
        split_high[pl.ds(e * 16, 16), :] = part
        split_low[pl.ds(e * 16, 16), :] = (block - part.astype(F32)).astype(BF16)
    for k in range(CAP):
        far_weights[k] = joined[step, jnp.maximum(target[k], 0)]
    wide = 256
    for n in range(0, field.shape[2], wide):
        cols = pl.ds(n, wide)
        s_high, s_low = split_high[:, cols], split_low[:, cols]
        w_high, w_low = high[step], low[step]
        total = jnp.dot(w_high, s_high, preferred_element_type=F32)
        total += jnp.dot(w_high, s_low, preferred_element_type=F32)
        total += jnp.dot(w_low, s_high, preferred_element_type=F32)
        for e in range(ELEMS):
            src = source[e, :, cols]
            least = jnp.min(src, axis=0, keepdims=True)
            most = jnp.max(src, axis=0, keepdims=True)
            moved[e, :, cols] = jnp.clip(total[e * 16 : e * 16 + 16], least, most)


def with_far(e, rows, cols, moved, far, is_far):
    t = moved[e, rows, cols]
    for k in range(CAP):
        t = jnp.where(is_far[k * ELEMS + e : k * ELEMS + e + 1, :] > 0.5, far[k, rows, cols], t)
    return t


def move_far(arrived, far_weights, moved, is_far, far, row_first, row_second):
    for k in range(CAP):
        src = arrived[k]
        s_high = src.astype(BF16)
        s_low = (src - s_high.astype(F32)).astype(BF16)
        total = jnp.dot(
            far_weights[k], jnp.concatenate([s_high, s_low, s_high], axis=0), preferred_element_type=F32
        )
        far[k] = jnp.clip(total, jnp.min(src, axis=0, keepdims=True), jnp.max(src, axis=0, keepdims=True))
    sub = sublane()
    flip = odd("face") == 1
    for n in range(0, moved.shape[2], 128):
        cols = slice(n, n + 128)
        packed = []
        for x, tile in ((0, 0), (3, 1)):
            rows = []
            for pair in range(2):
                at = slice(8 * tile, 8 * tile + 8)
                even = with_far(4 * x + 2 * pair, at, cols, moved, far, is_far)
                after = with_far(4 * x + 2 * pair + 1, at, cols, moved, far, is_far)
                if tile == 0:
                    rows.append(jnp.where(sub < 4, even, roll(after, 4)))
                else:
                    rows.append(jnp.where(sub < 4, roll(even, 4), after))
            left, right = rows
            inner = []
            for t in rows:
                t2 = jnp.where(sub == 3, 0.5 * (t + roll(t, 7)), t)
                inner.append(jnp.where(sub == 4, 0.5 * (t + roll(t, 1)), t2))
            inner[0] = jnp.where(sub == 7, 0.5 * (left + roll(right, 7)), inner[0])
            inner[1] = jnp.where(sub == 0, 0.5 * (right + roll(left, 1)), inner[1])
            packed.append(inner)
        for k in range(2):
            rows = slice(8 * k, 8 * k + 8)
            top, bottom = packed[0][k], packed[1][k]
            row_first[rows, cols] = jnp.where(flip, top, bottom)
            row_second[rows, cols] = jnp.where(flip, bottom, top)


def average_inside(moved, far, is_far, inside, left, right, draft, whole):
    sub = sublane()
    for e in range(ELEMS):
        for k in range(2):
            rows = slice(8 * k, 8 * k + 8)
            for n in range(0, moved.shape[2], 128):
                cols = slice(n, n + 128)
                whole[e, rows, cols] = with_far(e, rows, cols, moved, far, is_far)
    moved = whole
    first, last = sub % 4 == 0, sub % 4 == 3
    for e in range(ELEMS):
        y = e % 4
        for k in range(2):
            rows = slice(8 * k, 8 * k + 8)
            m = moved[e, rows, :]
            c = m
            if y < 3:
                c = jnp.where(last, 0.5 * (m + roll(moved[e + 1, rows, :], 3)), c)
            if y > 0:
                c = jnp.where(first, 0.5 * (m + roll(moved[e - 1, rows, :], 5)), c)
            draft[e, rows, :] = c
    for e in range(ELEMS):
        x = e // 4
        t0, t1 = draft[e, 0:8, :], draft[e, 8:16, :]
        if x > 0:
            t0 = jnp.where(sub < 4, 0.5 * (t0 + roll(draft[e - 4, 8:16, :], 4)), t0)
        if x < 3:
            t1 = jnp.where(sub >= 4, 0.5 * (t1 + roll(draft[e + 4, 0:8, :], 4)), t1)
        inside[e, 0:8, :] = t0
        inside[e, 8:16, :] = t1
    for out, y, at in ((left, 0, 0), (right, 3, 3)):
        for pair in range(2):
            packed = None
            for place in range(4):
                e = 4 * (2 * pair + place // 2) + y
                k = place % 2
                t = roll(inside[e, 8 * k : 8 * k + 8, :], place - at)
                packed = t if packed is None else jnp.where(sub % 4 == place, t, packed)
            out[8 * pair : 8 * pair + 8, :] = packed


def finish_columns(left, right, face_first, face_second, column_first, column_second):
    sub = sublane()
    flip = odd("face") == 1
    lo, hi = slice(0, 8), slice(8, 16)
    a0, a1, b0, b1 = (
        jnp.where(flip == from_first, face_first[rows, :], face_second[rows, :])
        for from_first in (True, False)
        for rows in (lo, hi)
    )
    l0 = jnp.where(sub == 0, 0.5 * (left[lo, :] + a0), left[lo, :])
    l1 = jnp.where(sub == 7, 0.5 * (left[hi, :] + roll(b0, 7)), left[hi, :])
    r0 = jnp.where(sub == 0, 0.5 * (right[lo, :] + roll(a1, 1)), right[lo, :])
    r1 = jnp.where(sub == 7, 0.5 * (right[hi, :] + b1), right[hi, :])
    flip = odd("tile") == 1
    for rows, l, r in ((lo, l0, r0), (hi, l1, r1)):
        column_first[rows, :] = jnp.where(flip, l, r)
        column_second[rows, :] = jnp.where(flip, r, l)


def finish_rows(inside, face_first, face_second, out):
    sub = sublane()
    flip = odd("face") == 1
    out[4:12] = inside[4:12]
    for y in range(4):
        first = face_first[8 * (y // 2) : 8 * (y // 2) + 8, :]
        second = face_second[8 * (y // 2) : 8 * (y // 2) + 8, :]
        a, b = jnp.where(flip, first, second), jnp.where(flip, second, first)
        t = inside[y, 0:8, :]
        out[y, 0:8, :] = jnp.where(sub < 4, 0.5 * (t + roll(a, 4 * (y % 2))), t)
        out[y, 8:16, :] = inside[y, 8:16, :]
        out[12 + y, 0:8, :] = inside[12 + y, 0:8, :]
        t = inside[12 + y, 8:16, :]
        out[12 + y, 8:16, :] = jnp.where(sub >= 4, 0.5 * (t + roll(b, 4 - 4 * (y % 2))), t)


def fix_edges(inside, tile_first, tile_second, put):
    sub = sublane()
    first, last = sub % 4 == 0, sub % 4 == 3
    flip = odd("tile") == 1
    for x in range(4):
        one = tile_first[8 * (x // 2) : 8 * (x // 2) + 8, :]
        two = tile_second[8 * (x // 2) : 8 * (x // 2) + 8, :]
        before, after = jnp.where(flip, one, two), jnp.where(flip, two, one)
        for k in range(2):
            place = 2 * (x % 2) + k
            rows = slice(8 * k, 8 * k + 8)
            t = inside[4 * x, rows, :]
            put(x, 0, rows, jnp.where(first, 0.5 * (t + roll(before, -place)), t))
            t = inside[4 * x + 3, rows, :]
            put(x, 1, rows, jnp.where(last, 0.5 * (t + roll(after, 3 - place)), t))


def finish_sends(listed, inside, tile_first, tile_second, *rest):
    sends, edges = rest[:4], rest[4]
    values = listed[...]

    def put(x, right, rows, t):
        edges[2 * x + right, rows, :] = t

    fix_edges(inside, tile_first, tile_second, put)
    for k in range(4):
        for c in range(CAP):
            e = values[k, c]
            y = e & 3
            at_edge = (y == 0) | (y == 3)
            place = 2 * (e >> 2) + (y >> 1)
            sends[k][c] = jnp.where(at_edge, edges[place], inside[e])


def finish_field(inside, tile_first, tile_second, field):
    def put(x, right, rows, t):
        field[4 * x + 3 * right, rows, :] = t

    fix_edges(inside, tile_first, tile_second, put)
    for x in range(4):
        field[4 * x + 1 : 4 * x + 3] = inside[4 * x + 1 : 4 * x + 3]


def finish_last(inside, tile_first, tile_second, field, edges, sems):
    copies = []
    for x in range(4):
        part = pl.ds(4 * x + 1, 2)
        copies.append(pltpu.make_async_copy(inside.at[part], field.at[part], sems.at[x]))
        copies[-1].start()

    def put(x, right, rows, t):
        edges[2 * x + right, rows, :] = t

    fix_edges(inside, tile_first, tile_second, put)
    for i in range(8):
        copies.append(
            pltpu.make_async_copy(edges.at[i], field.at[4 * (i // 2) + 3 * (i % 2)], sems.at[4 + i])
        )
        copies[-1].start()
    for copy in copies:
        copy.wait()


def swap(axis, slot, x):
    faces, tiles = lax.axis_size("face"), lax.axis_size("tile")
    pairs = []
    for f in range(faces):
        for t in range(tiles):
            if axis == "face":
                step = 1 if (f + t + slot) % 2 == 0 else -1
                target = (f + step) % faces * tiles + t
            else:
                step = 1 if (t + slot) % 2 == 0 else -1
                target = f * tiles + (t + step) % tiles
            pairs.append((f * tiles + t, target))
    return lax.ppermute(x, ("face", "tile"), pairs)


def swaps(axis, first, second):
    return swap(axis, 0, first), swap(axis, 1, second)


def odd(axis):
    place = lax.axis_index("tile")
    if axis == "face":
        place += lax.axis_index("face")
    return lax.rem(place, 2)


def transport(tracers, basis_weights, up_owner, up_slot, send_list):
    columns = tracers.shape[3]
    steps = basis_weights.shape[0]
    block = jax.ShapeDtypeStruct((ELEMS, NODES, columns), F32)
    edge = jax.ShapeDtypeStruct((16, columns), F32)
    listed = jax.ShapeDtypeStruct((CAP, NODES, columns), F32)
    mats = jax.ShapeDtypeStruct((steps, 256, 256), BF16)
    own = jax.ShapeDtypeStruct((steps, 16, 16, 48), BF16)
    far_own = jax.ShapeDtypeStruct((CAP, 16, 48), BF16)
    own_lists = jax.ShapeDtypeStruct((8, 128), jnp.int32)
    flags = jax.ShapeDtypeStruct((CAP * ELEMS, 128), F32)
    table = pltpu.SMEM(
        (min(8, send_list.shape[1]), 128 if send_list.shape[2] % 128 == 0 else send_list.shape[2]), jnp.int32
    )
    field = tracers.reshape(ELEMS, NODES, columns)
    weights = basis_weights.reshape(steps, 256, 16)

    lists_hbm = pltpu.with_memory_space_constraint(send_list, pltpu.HBM)
    field_hbm = pltpu.with_memory_space_constraint(field, pltpu.HBM)
    whole = pltpu.VMEM(block.shape, F32)
    edges = pltpu.VMEM((8, NODES, columns), F32)
    halves = pltpu.VMEM((256, columns), BF16)
    dma = pltpu.SemaphoreType.DMA
    *sends, field = run(first_gather, [HBM, HBM], [listed] * 4 + [block], 1, [table, dma, dma], lists_hbm, field_hbm)
    high, low, joined = run(spread_weights, [VMEM], [mats, mats, own], 1, [], weights)
    for step in range(steps):
        face = swaps("face", sends[0], sends[1])
        tile = swaps("tile", sends[2], sends[3])
        if step < steps - 1:
            upcoming = run(functools.partial(read_lists, step + 1), [HBM], own_lists, 1, [table, dma], lists_hbm)
        if step > 0:
            field = run(finish_field, [VMEM] * 3, block, 2, [], inside, *edge_tile)
        blocks = [*face, *tile]
        last = blocks.pop(LAST)
        moved, far_weights, is_far = run(
            functools.partial(move_most, step), [SMEM, SMEM] + [VMEM] * 7,
            [block, far_own, flags], 5, [whole, halves, halves],
            up_owner, up_slot, field, *blocks, high, low, joined,
        )
        far, *rows = run(move_far, [VMEM] * 4, [listed, edge, edge], 1, [], last, far_weights, moved, is_far)
        edge_face = swaps("face", *rows)
        inside, left, right = run(
            average_inside, [VMEM] * 3, [block, edge, edge], 3, [whole, whole],
            moved, far, is_far,
        )
        ends = run(finish_columns, [VMEM] * 4, [edge] * 2, 1, [], left, right, *edge_face)
        edge_tile = swaps("tile", *ends)
        inside = run(finish_rows, [VMEM] * 3, block, 1, [], inside, *edge_face)
        if step < steps - 1:
            sends = run(finish_sends, [VMEM] * 4, [listed] * 4, 2, [edges], upcoming, inside, *edge_tile)
        else:
            field = run(
                finish_last, [VMEM] * 3, block, 2, [edges, dma((12,))], inside, *edge_tile,
                out_space=HBM,
            )
    return field.reshape(tracers.shape)


def solution(mesh):
    return jax.shard_map(
        transport,
        mesh=mesh,
        in_specs=(
            P("face", "tile", None, None),
            P(None, "face", "tile", None, None),
            P(None, "face", "tile"),
            P(None, "face", "tile"),
            P(),
        ),
        out_specs=P("face", "tile", None, None),
        check_vma=False,
    )
```
